128 devices in a mesh: gx: 16 (over y, z), gy: 8 (over x, core).
Axes of the slice: x: 4, y: 4, z: 4, core: 2. Of those that a mesh axis runs over, the one named last changes fastest.
Arguments:
- snapshots: bfloat16 [16, 16, 4, 2048, 512], P('gx', 'gy'), may hold values from -120 to 120
- basis: bfloat16 [16, 16, 4, 24, 2048], P('gx', 'gy'), may hold values from -0.0625 to 0.0625
- node_counts: int32 [16, 16], P('gx', 'gy'), may hold values from 1024 to 2048, as said below
- adjacency: int32 [16, 16, 3], P('gx', 'gy'), may hold values from 0 to 255, as said below
Outputs:
- operator: float32 [16, 16, 397, 24], P('gx', 'gy')
- reduced_states: float32 [16, 16, 24, 512], P('gx', 'gy')
The draws below stay inside these ranges and needn't reach their ends.
Inputs may be any that keep to these rules, and one draw needn't show every extreme that they name: Node slot n of subdomain g is live iff n < node_counts[g]; at least 1024 slots are live, and one subdomain has all 2048 live. Subdomain (row, col) has id row * 16 + col. Each row of adjacency holds 3 distinct ids other than its own subdomain's, each within one subdomain row and one subdomain column of it.
All inputs are finite; a program needn't handle non-finite values.
Results may differ from the reference program's by a relative error of at most 0.0003.
Values sent between devices are 32-bit elements; how exact they have to be, the bound alone decides.
A program may use at most 64 MiB of HBM per device.

```python
import jax
import jax.numpy as jnp
import numpy as np
from jax import lax

R = 24
NVAR = 4
K = 512
P_SIZE = 2048
NB = 3
GRID_R = 16
GRID_C = 16
NF = 397


def draw_node_counts(key, part):
    first, second = jax.random.split(jax.random.fold_in(key, 11))
    counts = jax.random.randint(first, (GRID_R * GRID_C,), P_SIZE // 2, P_SIZE + 1, dtype=jnp.int32)
    where_full = jax.random.randint(second, (), 0, GRID_R * GRID_C, dtype=jnp.int32)
    counts = jnp.where(jnp.arange(GRID_R * GRID_C, dtype=jnp.int32) == where_full, P_SIZE, counts)
    return counts.reshape(GRID_R, GRID_C).astype(jnp.int32)


def draw_adjacency(key, part):
    offsets = np.array([(a, b) for a in range(-1, 2) for b in range(-1, 2)], dtype=np.int32)
    rows = jnp.arange(GRID_R, dtype=jnp.int32)[:, None, None]
    cols = jnp.arange(GRID_C, dtype=jnp.int32)[None, :, None]
    near_rows = jnp.broadcast_to(rows + jnp.asarray(offsets[:, 0]), (GRID_R, GRID_C, 9))
    near_cols = jnp.broadcast_to(cols + jnp.asarray(offsets[:, 1]), (GRID_R, GRID_C, 9))
    inside = (near_rows >= 0) & (near_rows < GRID_R) & (near_cols >= 0) & (near_cols < GRID_C)
    itself = (near_rows == rows) & (near_cols == cols)
    scores = jax.random.randint(jax.random.fold_in(key, 13), (GRID_R, GRID_C, 9), 0, 1000, dtype=jnp.int32) * 16 + jnp.arange(9, dtype=jnp.int32)
    scores = jnp.where(inside & jnp.logical_not(itself), scores, -1)
    unused, picked = lax.top_k(scores, NB)
    chosen_rows = jnp.take_along_axis(near_rows, picked, axis=2)
    chosen_cols = jnp.take_along_axis(near_cols, picked, axis=2)
    return (chosen_rows * GRID_C + chosen_cols).astype(jnp.int32)


def draw_snapshots(key, part):
    keys = jax.random.split(jax.random.fold_in(key, 17), 3)
    shape = (GRID_R, GRID_C, NVAR, P_SIZE, K)
    ident = jnp.arange(GRID_R * GRID_C, dtype=jnp.float32).reshape(GRID_R, GRID_C) / max(GRID_R * GRID_C - 1, 1)
    var_scale = jnp.exp(jax.random.uniform(keys[0], (NVAR,), jnp.float32, jnp.log(0.5), jnp.log(4.0)))
    rough = jax.random.uniform(keys[1], (GRID_R, GRID_C, NVAR, P_SIZE, 1), jnp.float32, 0.5, 1.5)
    base = jnp.clip(jax.random.normal(keys[2], shape, jnp.float32), -6.0, 6.0)
    rise = 1.0 + 2.0 * ident
    values = base * rough * var_scale[None, None, :, None, None] * rise[:, :, None, None, None]
    return values.astype(jnp.bfloat16)


def shard_levels(rng, shape, shards, least, top_value):
    loudness, own = 1.0, jax.random.fold_in(rng, 6)
    for position, parts in shards:
        steps = jnp.exp(jax.random.uniform(jax.random.fold_in(own, position), (parts,), jnp.float32, least / len(shards), top_value / len(shards)))
        loudness = loudness * jnp.repeat(steps, shape[position] // parts).reshape([-1 if axis == position else 1 for axis in range(len(shape))])
    return loudness


def gaussian(own_key, shape, deviation, reach, cuts=(), kind=jnp.bfloat16):
    result = jax.random.normal(own_key, shape, jnp.float32) * deviation
    if len(cuts) > 0:
        result = shard_levels(own_key, shape, cuts, -0.22, 0.18) * result
    return jnp.clip(result, min=-reach, max=reach).astype(kind)


def setup_inputs(seed: int = 0) -> dict:
    seeds = jax.random.split(jax.random.key(seed), 5)
    return {
        "snapshots": draw_snapshots(jax.random.fold_in(seeds[4], 71), 0),
        "basis": gaussian(seeds[1], (GRID_R, GRID_C, NVAR, R, P_SIZE), (NVAR * P_SIZE) ** -0.5, 0.0625, ((0, 16), (1, 8))),
        "node_counts": draw_node_counts(jax.random.fold_in(seeds[4], 71), 0),
        "adjacency": draw_adjacency(jax.random.fold_in(seeds[4], 71), 0),
    }


beta_linear = 0.5
beta_quad = 0.5

def project_one(items):
    values, modes, count = items
    live = (jnp.arange(values.shape[1], dtype=jnp.int32) < count).astype(jnp.float32)
    masked = modes.astype(jnp.float32) * live[None, None, :]
    proj = jnp.einsum('vrp,vpk->vrk', masked, values.astype(jnp.float32), precision=lax.Precision.HIGHEST)
    valf = values.astype(jnp.float32)
    squares = lax.optimization_barrier(jnp.sum(valf * valf * live[None, :, None], axis=(1, 2)))
    return (proj, squares)

def build_features(state, near):
    ranks = state.shape[0]
    steps = state.shape[1]
    pieces = [jnp.ones((1, steps), jnp.float32), state, near.reshape(-1, steps)]
    for first in range(ranks):
        pieces.append(state[first:first + 1] * state[first:])
    return jnp.concatenate(pieces, axis=0)

def fit_one(state, near, reg_diag):
    feats = build_features(state, near)
    past = feats[:, :-1]
    gram = jnp.dot(past, past.T, precision=lax.Precision.HIGHEST) + jnp.diag(reg_diag)
    rhs = jnp.dot(past, state[:, 1:].T, precision=lax.Precision.HIGHEST)
    factor = jnp.linalg.cholesky(gram)
    middle = jax.scipy.linalg.solve_triangular(factor, rhs, lower=True)
    return jax.scipy.linalg.solve_triangular(factor, middle, lower=True, trans=1)

def reference(snapshots, basis, node_counts, adjacency):
    grid_rows, grid_cols = (snapshots.shape[0], snapshots.shape[1])
    total = grid_rows * grid_cols
    values = snapshots.reshape(total, NVAR, P_SIZE, K)
    modes = basis.reshape(total, NVAR, R, P_SIZE)
    counts = node_counts.reshape(total).astype(jnp.int32)
    proj, squares = lax.map(project_one, (values, modes, counts))
    nodes = jnp.sum(counts.astype(jnp.float32))
    scale = jnp.sqrt(lax.optimization_barrier(jnp.sum(squares, axis=0)) / (nodes * K) + 1e-06)
    states = lax.optimization_barrier(jnp.sum(proj / scale[None, :, None, None], axis=1))
    gnorm = jnp.sum(states * states) / (total * R * K)
    near = states[adjacency.reshape(total, NB).astype(jnp.int32)]
    nlin = 1 + R + NB * R
    nquad = R * (R + 1) // 2
    reg_diag = K * jnp.concatenate([jnp.full((nlin,), beta_linear, jnp.float32) * gnorm, jnp.full((nquad,), beta_quad, jnp.float32) * gnorm * gnorm])
    operator = lax.map(lambda items: fit_one(items[0], items[1], reg_diag), (states, near))
    return (operator.reshape(grid_rows, grid_cols, NF, R), states.reshape(grid_rows, grid_cols, R, K))
```

```python
import functools

import jax
import jax.numpy as jnp
from jax import lax
from jax.experimental import pallas as pl
from jax.experimental.pallas import tpu as pltpu
from jax.sharding import PartitionSpec as P

MESH = pl.DeviceIdType.MESH
F32 = jnp.float32
BF16 = jnp.bfloat16
R = 24
NV = 4
PAIRS = [(v, w) for v in range(NV) for w in range(v, NV)]
ROWS = 400
QUAD_END = 300
OWN = 304
NEAR = 328
HALF = 64


def feature_rows():
    place = {}
    for a in range(3):
        for r in range(4):
            for m in range(8):
                i, j = 8 * a + m, 8 * a + (m + r) % 8
                place[(min(i, j), max(i, j))] = (4 * a + r) * 8 + m
    for c, (a, b) in enumerate(((0, 1), (0, 2), (1, 2))):
        for r in range(8):
            for m in range(8):
                place[(8 * a + m, 8 * b + (m + r) % 8)] = (12 + 8 * c + r) * 8 + m
    for m in range(4):
        place[(m, m + 4)] = 288 + m
        place[(8 + m, 12 + m)] = 292 + m
        place[(16 + m, 20 + m)] = 296 + m
    rows = [QUAD_END] + list(range(OWN, OWN + R)) + list(range(NEAR, NEAR + 3 * R))
    for i in range(R):
        for j in range(i, R):
            rows.append(place[(i, j)])
    return rows


SOURCE = feature_rows()


def iota(shape, dim):
    return lax.broadcasted_iota(jnp.int32, shape, dim)


def split2(x):
    hi = x.astype(BF16)
    return hi, (x - hi.astype(F32)).astype(BF16)


def mm(a, b):
    return jnp.dot(a, b, preferred_element_type=F32)


def mm_nt(a, b):
    return lax.dot_general(a, b, (((1,), (1,)), ((), ())), preferred_element_type=F32)


def scan_kernel(counts_ref, vals_ref, modes_ref, proj_ref, stats_ref, acc_ref):
    s = pl.program_id(0)
    v = pl.program_id(1)
    count = counts_ref[0, s]
    slots = vals_ref.shape[0]

    @pl.when((s == 0) & (v == 0))
    def _():
        acc_ref[...] = jnp.zeros_like(acc_ref)

    lanes = iota((R, slots), 1)
    modes = jnp.where(lanes < count, modes_ref[...].astype(F32), 0.0).astype(BF16)
    proj_ref[pl.ds(v, 1)] = mm(modes, vals_ref[...])[None]
    chunk = 128

    def step(c, acc):
        x = vals_ref[pl.ds(pl.multiple_of(c * chunk, chunk), chunk), :].astype(F32)
        rows = iota((chunk, x.shape[1]), 0) + c * chunk
        x = jnp.where(rows < count, x, 0.0)
        x = x * x
        x = jnp.sum(x.reshape(chunk // 8, 8, x.shape[1]), axis=0)
        return acc + x

    sq = lax.fori_loop(0, slots // chunk, step, jnp.zeros((8, vals_ref.shape[1]), F32))
    sq = sq[:, 0:128] + sq[:, 128:256] + sq[:, 256:384] + sq[:, 384:512]
    acc_ref[pl.ds(v, 1)] += sq[None]

    @pl.when(v == NV - 1)
    def _():
        for n, (a, b) in enumerate(PAIRS):
            x = proj_ref[a] * proj_ref[b]
            x = x[0:8] + x[8:16] + x[16:24]
            acc_ref[NV + n] += x[:, 0:128] + x[:, 128:256] + x[:, 256:384] + x[:, 384:512]

    @pl.when((s == 1) & (v == NV - 1))
    def _():
        rows = [jnp.sum(acc_ref[n], axis=0, keepdims=True) for n in range(NV + len(PAIRS))]
        rows += [jnp.zeros((1, 128), F32)] * (16 - len(rows))
        table = jnp.concatenate(rows, axis=0)
        col = jnp.sum(table, axis=1, keepdims=True)
        spread = jnp.where(iota((16, 128), 0) == iota((16, 128), 1), col, 0.0)
        line = jnp.sum(spread, axis=0, keepdims=True)
        nodes = (counts_ref[0, 0] + counts_ref[0, 1]).astype(F32)
        stats_ref[...] = jnp.where(iota((1, 128), 1) == 15, nodes, line)


def exchange_kernel(nx, ny, total, proj_ref, stats_ref, halo_ref, gnorm_ref,
                    near, slot1, slot2, send1, recv1, send2, recv2, hs, hr):
    gx = lax.axis_index("gx")
    gy = lax.axis_index("gy")
    barrier = pltpu.get_barrier_semaphore()
    for d in range(1, ny):
        pl.semaphore_signal(barrier, inc=1, device_id=(gx, lax.rem(gy + d, ny)), device_id_type=MESH)
    for d in range(1, nx):
        pl.semaphore_signal(barrier, inc=1, device_id=(lax.rem(gx + d, nx), gy), device_id_type=MESH)
    pl.semaphore_wait(barrier, nx + ny - 2)

    slot1[0] = stats_ref[...]
    copies = []
    for d in range(1, ny):
        c = pltpu.make_async_remote_copy(
            src_ref=slot1.at[0], dst_ref=slot1.at[d], send_sem=send1.at[d], recv_sem=recv1.at[d],
            device_id=(gx, lax.rem(gy + d, ny)), device_id_type=MESH)
        c.start()
        copies.append(c)
    for c in copies:
        c.wait()
    part = [slot1[lax.rem(gy - n + ny, ny)] for n in range(ny)]
    line = part[0]
    for x in part[1:]:
        line = line + x
    slot2[0] = line
    copies = []
    for d in range(1, nx):
        c = pltpu.make_async_remote_copy(
            src_ref=slot2.at[0], dst_ref=slot2.at[d], send_sem=send2.at[d], recv_sem=recv2.at[d],
            device_id=(lax.rem(gx + d, nx), gy), device_id_type=MESH)
        c.start()
        copies.append(c)
    for c in copies:
        c.wait()
    part = [slot2[lax.rem(gx - n + nx, nx)] for n in range(nx)]
    line = part[0]
    for x in part[1:]:
        line = line + x

    lane = iota((1, 128), 1)

    def pick(n):
        return jnp.sum(jnp.where(lane == n, line, 0.0), axis=1, keepdims=True)

    nodes = pick(15)
    steps = proj_ref.shape[-1]
    inv = [1.0 / jnp.sqrt(pick(v) / (nodes * steps) + 1e-06) for v in range(NV)]
    g = jnp.zeros((1, 1), F32)
    for n, (a, b) in enumerate(PAIRS):
        g = g + (1.0 if a == b else 2.0) * pick(NV + n) * inv[a] * inv[b]
    gnorm_ref[...] = jnp.broadcast_to(g / (total * R * steps), (1, 128))
    for s in range(2):
        x = proj_ref[s, 0] * inv[0]
        for v in range(1, NV):
            x = x + proj_ref[s, v] * inv[v]
        near[1, 1 + s] = x
    up, down = lax.rem(gx + 1, nx), lax.rem(gx + nx - 1, nx)
    right, left = lax.rem(gy + 1, ny), lax.rem(gy + ny - 1, ny)

    def send(n, src, dst, dev):
        return pltpu.make_async_remote_copy(
            src_ref=src, dst_ref=dst, send_sem=hs.at[n], recv_sem=hr.at[n], device_id=dev, device_id_type=MESH)

    own = near.at[1, pl.ds(1, 2)]
    one = send(0, own, near.at[0, pl.ds(1, 2)], (up, gy))
    two = send(1, own, near.at[2, pl.ds(1, 2)], (down, gy))
    one.start()
    two.start()
    one.wait()
    two.wait()
    three = send(2, near.at[:, 2], near.at[:, 0], (gx, right))
    four = send(3, near.at[:, 1], near.at[:, 3], (gx, left))
    three.start()
    four.start()
    three.wait()
    four.wait()
    halo_ref[...] = near[...]


def invert_block(x_ref, panels):
    lane = iota((8, 128), 1)
    sub = iota((8, 128), 0)
    inner = lane % HALF
    half = lane - inner

    def panel(p, carry):
        off = p * 8
        xs = [x_ref[8 * i:8 * i + 8, :] for i in range(panels)]
        rb = x_ref[pl.ds(pl.multiple_of(off, 8), 8), :]
        idx = [half + off + l for l in range(8)]
        c = [jnp.take_along_axis(rb, idx[l], axis=1) for l in range(8)]
        for k in range(8):
            r = 1.0 / jnp.broadcast_to(c[k][k:k + 1, :], (8, 128))
            f = jnp.where(sub == k, -r, c[k] * r)
            new = []
            for j in range(8):
                if j == k:
                    new.append(-f)
                else:
                    t = jnp.broadcast_to(c[j][k:k + 1, :], (8, 128))
                    new.append(jnp.where(sub == k, 0.0, c[j]) - f * t)
            c = new
        inp = (inner >= off) & (inner < off + 8)
        rb = jnp.where(inp, jnp.where(inner - off == sub, 1.0, 0.0), rb)
        prods = [c[l] * jnp.broadcast_to(rb[l:l + 1, :], (8, 128)) for l in range(8)]
        while len(prods) > 1:
            prods = [prods[i] + prods[i + 1] for i in range(0, len(prods), 2)]
        q = prods[0]
        qb = [jnp.broadcast_to(q[l:l + 1, :], (8, 128)) for l in range(8)]
        for i in range(panels):
            prods = [jnp.take_along_axis(xs[i], idx[l], axis=1) * qb[l] for l in range(8)]
            while len(prods) > 1:
                prods = [prods[n] + prods[n + 1] for n in range(0, len(prods), 2)]
            x_ref[8 * i:8 * i + 8, :] = jnp.where(inp, 0.0, xs[i]) - prods[0]
        x_ref[pl.ds(pl.multiple_of(off, 8), 8), :] = q
        return carry

    lax.fori_loop(0, panels, panel, 0)


def fit_kernel(gy_size, grid_cols, adj_ref, halo_ref, gnorm_ref, op_ref, st_ref,
               hi_ref, lo_ref, a_ref, x_ref, y_ref):
    gx = lax.axis_index("gx")
    gy = lax.axis_index("gy")
    g = gnorm_ref[0:1, 0:1]
    rg = 1.0 / jnp.sqrt(g)
    steps = halo_ref.shape[-1]
    keep = iota((8, steps), 1) < steps - 1
    sub = iota((8, steps), 0)
    for s in range(2):
        own = halo_ref[1, 1 + s]
        st_ref[s] = own
        t = own * rg
        future = pltpu.roll(t, steps - 1, axis=1)
        tile = [jnp.where(keep, t[8 * a:8 * a + 8], 0.0) for a in range(3)]

        def put(n, x):
            hi, lo = split2(x)
            hi_ref[s, 8 * n:8 * n + x.shape[0], :] = hi
            lo_ref[s, 8 * n:8 * n + x.shape[0], :] = lo

        def turned(x, r):
            return pltpu.roll(x, 8 - r, axis=0) if r else x

        tiles = []
        for a in range(3):
            for r in range(4):
                tiles.append(tile[a] * turned(tile[a], r))
        for a, b in ((0, 1), (0, 2), (1, 2)):
            for r in range(8):
                tiles.append(tile[a] * turned(tile[b], r))
        opp = [tile[a] * turned(tile[a], 4) for a in range(3)]
        tiles.append(jnp.where(sub < 4, opp[0], opp[1]))
        one = jnp.where((sub == 4) & keep, jnp.broadcast_to(rg, (8, steps)), 0.0)
        tiles.append(jnp.where(sub < 4, opp[2], one))
        tiles += tile
        for b in range(3):
            node = adj_ref[0, s, b]
            row = node // grid_cols - gx + 1
            col = node % grid_cols - gy * 2 + 1
            x = halo_ref[row, col] * rg
            for a in range(3):
                tiles.append(jnp.where(keep, x[8 * a:8 * a + 8], 0.0))
        tiles += [future[8 * a:8 * a + 8] for a in range(3)]
        tiles.append(jnp.zeros((8, steps), F32))
        for n in range(0, len(tiles), 2):
            put(n, jnp.concatenate(tiles[n:n + 2], axis=0))
        top = 8 * len(tiles)
        hi_ref[s, top:512, :] = jnp.zeros((512 - top, steps), BF16)
        lo_ref[s, top:512, :] = jnp.zeros((512 - top, steps), BF16)

        for n in range(2):
            cols = slice(256 * n, 256 * n + 256)
            x = (mm_nt(hi_ref[s, 0:ROWS, :], hi_ref[s, cols, :])
                 + mm_nt(lo_ref[s, 0:ROWS, :], hi_ref[s, cols, :])
                 + mm_nt(hi_ref[s, 0:ROWS, :], lo_ref[s, cols, :]))
            diag = iota((ROWS, 256), 0) == iota((ROWS, 256), 1) + 256 * n
            a_ref[s, :, cols] = x + jnp.where(diag, 0.5 * steps, 0.0)

    lane = iota((8, 128), 1)
    for k in range(7):
        top = HALF * k
        size = min(HALF, ROWS - top)
        tile = k // 2
        odd = k % 2
        start = 128 * ((k + 1) // 2)
        rows = slice(top, top + size)
        left = lane[0:1] < HALF
        xa = a_ref[0, rows, 128 * tile:128 * tile + 128]
        xb = a_ref[1, rows, 128 * tile:128 * tile + 128]
        if odd:
            xa = pltpu.roll(xa, HALF, axis=1)
        else:
            xb = pltpu.roll(xb, HALF, axis=1)
        x_ref[0:size, :] = jnp.where(left, xa, xb)
        invert_block(x_ref, size // 8)
        xh, xl = split2(x_ref[0:size, :])
        for s in range(2):
            bh, bl = split2(a_ref[s, rows, start:512])
            zero = jnp.zeros((HALF, 512 - start), BF16)
            fill = jnp.zeros((HALF - size, 512 - start), BF16)

            def stack(b, second):
                parts = [b] if size == HALF else [b, fill]
                return jnp.concatenate([zero] + parts if second else parts + [zero], axis=0)

            bh, bl = stack(bh, s == 1), stack(bl, s == 1)
            w = mm(xh, bh) + mm(xl, bh) + mm(xh, bl)
            wh, wl = split2(w)
            wh, wl = stack(wh, odd), stack(wl, odd)
            ch, cl = split2(a_ref[s, :, 128 * tile:128 * tile + 128])
            a_ref[s, :, start:512] -= mm(ch, wh) + mm(cl, wh) + mm(ch, wl)
            a_ref[s, rows, start:512] = w

    for s in range(2):
        y = pltpu.roll(a_ref[s, :, 384:512], 128 - (ROWS - 384), axis=1)
        quad = iota((ROWS, 128), 0) < QUAD_END
        y_ref[...] = jnp.where(quad, y * rg, y)
        for n, m in enumerate(SOURCE):
            op_ref[s, n:n + 1, :] = y_ref[m:m + 1, 0:R]


def scan_call(snapshots, basis, counts):
    _, subs, nv, slots, steps = snapshots.shape
    return pl.pallas_call(
        scan_kernel,
        grid=(subs, nv),
        in_specs=[
            pl.BlockSpec(memory_space=pltpu.SMEM),
            pl.BlockSpec((None, None, None, slots, steps), lambda s, v: (0, s, v, 0, 0)),
            pl.BlockSpec((None, None, None, R, slots), lambda s, v: (0, s, v, 0, 0)),
        ],
        out_specs=[
            pl.BlockSpec((None, nv, R, steps), lambda s, v: (s, 0, 0, 0)),
            pl.BlockSpec((1, 128), lambda s, v: (0, 0)),
        ],
        out_shape=[
            jax.ShapeDtypeStruct((subs, nv, R, steps), F32),
            jax.ShapeDtypeStruct((1, 128), F32),
        ],
        scratch_shapes=[pltpu.VMEM((16, 8, 128), F32)],
        compiler_params=pltpu.CompilerParams(dimension_semantics=("arbitrary", "arbitrary")),
        name="scan",
    )(counts, snapshots, basis)


def exchange_call(proj, stats, nx, ny, total):
    steps = proj.shape[-1]
    vm = pl.BlockSpec(memory_space=pltpu.VMEM)
    dma = pltpu.SemaphoreType.DMA
    return pl.pallas_call(
        functools.partial(exchange_kernel, nx, ny, total),
        in_specs=[vm, vm],
        out_specs=[vm, vm],
        out_shape=[
            jax.ShapeDtypeStruct((3, 4, R, steps), F32),
            jax.ShapeDtypeStruct((1, 128), F32),
        ],
        scratch_shapes=[
            pltpu.VMEM((3, 4, R, steps), F32),
            pltpu.VMEM((ny, 1, 128), F32),
            pltpu.VMEM((nx, 1, 128), F32),
            dma((ny,)), dma((ny,)), dma((nx,)), dma((nx,)), dma((4,)), dma((4,)),
        ],
        compiler_params=pltpu.CompilerParams(collective_id=0, has_side_effects=True),
        name="exchange",
    )(proj, stats)


def fit_call(adj, halo, gnorm, ny):
    steps = halo.shape[-1]
    vm = pl.BlockSpec(memory_space=pltpu.VMEM)
    return pl.pallas_call(
        functools.partial(fit_kernel, ny, 2 * ny),
        in_specs=[pl.BlockSpec(memory_space=pltpu.SMEM), vm, vm],
        out_specs=[vm, vm],
        out_shape=[
            jax.ShapeDtypeStruct((2, 397, R), F32),
            jax.ShapeDtypeStruct((2, R, steps), F32),
        ],
        scratch_shapes=[
            pltpu.VMEM((2, 512, steps), BF16),
            pltpu.VMEM((2, 512, steps), BF16),
            pltpu.VMEM((2, ROWS, 512), F32),
            pltpu.VMEM((HALF, 128), F32),
            pltpu.VMEM((ROWS, 128), F32),
        ],
        name="fit",
    )(adj, halo, gnorm)


def solution(mesh):
    nx, ny = mesh.shape["gx"], mesh.shape["gy"]

    def body(snapshots, basis, counts, adj):
        proj, stats = scan_call(snapshots, basis, counts)
        total = nx * ny * snapshots.shape[1]
        halo, gnorm = exchange_call(proj, stats, nx, ny, total)
        op, st = fit_call(adj, halo, gnorm, ny)
        return op[None], st[None]

    lead = P("gx", "gy")
    return jax.shard_map(
        body,
        mesh=mesh,
        in_specs=(lead, lead, lead, lead),
        out_specs=(lead, lead),
        check_vma=False,
    )
```
